32 devices in a mesh: dp: 8 (over z, core), vocab: 4 (over y, x).
Axes of the slice: x: 2, y: 2, z: 4, core: 2. Of those that a mesh axis runs over, the one named last changes fastest.
Arguments:
- hidden: bfloat16 [2, 8, 128, 2048], P(None, 'dp'), may hold values from -320 to 320
- out_weight: bfloat16 [2048, 51200], P('dp', 'vocab'), may hold values from -1 to 1
- targets: int32 [2, 8, 128], P(None, 'dp'), may hold values from 0 to 51199
- prompt_start: int32 [2, 8], P(None, 'dp'), may hold values from 0 to 31
- response_len: int32 [2, 8], P(None, 'dp'), may hold values from 16 to 80, as said below
- partner: int32 [2, 8], P(None, 'dp'), may hold values from 0 to 7, as said below
- ref_scores: float32 [2, 8], P(None, 'dp'), may hold values from -60 to 60
Outputs:
- pair_loss: float32 [2, 8], P(None, 'dp')
- grad_hidden: float32 [2, 8, 128, 2048], P(None, 'dp', None, 'vocab')
The draws below stay inside these ranges and needn't reach their ends.
Inputs may be any that keep to these rules, and one draw needn't show every extreme that they name: In each microbatch partner pairs the sequences: the partner of the partner of s is s, and it differs from s. `response_len`: the response length of sequence s is below 17 + 64 * (s + 1) // 8.
All inputs are finite; a program needn't handle non-finite values.
Results may differ from the reference program's by a relative error of at most 0.0059.
Values may be sent and summed in bfloat16 or wider, within the bound.
No kernel may reach another device: no remote copies, remote signals or barrier semaphores. Data moves between devices by JAX's collectives and lax.ppermute only.
A program may use at most 128 MiB of HBM per device.

```python
import math
import jax
import jax.numpy as jnp
import numpy as np
from jax import lax

D = 2048
VOC = 51200
MB = 2
L = 128
SEQS = 8


def common_direction(key):
    shared = jax.random.normal(jax.random.fold_in(key, 9173), (D,), jnp.float32)
    return jnp.clip(shared, -4.0, 4.0) / jnp.sqrt(jnp.float32(D))


def draw_out_weight(key, part):
    direction = common_direction(key)
    noise = jax.random.normal(jax.random.fold_in(key, 4421), (D, VOC), jnp.float32)
    values = jnp.clip(noise, -4.0, 4.0) / jnp.sqrt(jnp.float32(D)) + direction[:, None]
    return values.astype(jnp.bfloat16)


def draw_hidden(key, part):
    direction = common_direction(key)
    key_base = jax.random.fold_in(key, 11)
    key_row = jax.random.fold_in(key, 15)
    key_shift = jax.random.fold_in(key, 16)
    values = jax.random.normal(key_base, (MB, SEQS, L, D), jnp.float32)
    shift_row = jax.random.randint(key_row, (MB, SEQS, 1), 0, L)
    position = jnp.arange(L, dtype=jnp.int32)[None, None, :]
    shift_levels = jnp.array([120.0, 200.0, 280.0], jnp.float32)
    shift = shift_levels[jax.random.randint(key_shift, (MB, SEQS, 1), 0, 3)]
    shift = jnp.where(position == shift_row, shift, 0.0)
    unit = direction / jnp.sum(direction * direction)
    values = values + shift[..., None] * unit[None, None, None, :]
    return jnp.clip(values, -320.0, 320.0).astype(jnp.bfloat16)


def draw_response_len(key, part):
    lowest = L // 8
    index = jnp.arange(SEQS, dtype=jnp.int32)
    upper_end = lowest + 1 + L // 2 * (index + 1) // SEQS
    lengths = jax.random.randint(key, (MB, SEQS), lowest, upper_end[None, :], dtype=jnp.int32)
    lengths = lengths.at[0, SEQS - 1].set(jnp.int32(lowest + L // 2))
    return lengths.at[0, 0].set(jnp.int32(lowest))


def draw_partner(key, part):

    def one_batch(batch_key):
        order = jax.random.permutation(batch_key, SEQS).astype(jnp.int32)
        paired = jnp.zeros((SEQS,), jnp.int32)
        paired = paired.at[order[0::2]].set(order[1::2])
        return paired.at[order[1::2]].set(order[0::2])
    return jax.vmap(one_batch)(jax.random.split(key, MB))


def place_ends(result, stream_key, low, largest):
    longest = result.shape.index(max(result.shape))
    spots = []
    for shift in (0, 1):
        where = [jax.random.randint(jax.random.fold_in(stream_key, axis), (), 0, length) for axis, length in enumerate(result.shape)]
        where[longest] = (where[longest] + shift) % result.shape[longest]
        spots.append(tuple(where))
    return result.at[spots[0]].set(low).at[spots[1]].set(largest)


def level_of(stream_key, dims, shards, smallest, high):
    def one(axis_at, shards_of):
        steps = jax.random.uniform(jax.random.fold_in(jax.random.fold_in(stream_key, 6), axis_at), (shards_of,), jnp.float32, smallest / len(shards), high / len(shards))
        return jnp.repeat(jnp.exp(steps), dims[axis_at] // shards_of).reshape((-1,) + (1,) * (len(dims) - axis_at - 1))

    gain = one(*shards[0])
    for cut in shards[1:]:
        gain = gain * one(*cut)
    return gain


def rank_table(amount, lean):
    portions = [(1 << 20) // math.isqrt(grade ** lean) + 1 for grade in range(1, amount + 1)]
    width = 1 + sum(portions) // (1 << 30)
    return np.cumsum(np.array([max(1, weight // width) for weight in portions]))


def ranked_ids(own_key, dims, amount, skew):
    grid = rank_table(amount, skew)
    ticket = jax.random.randint(jax.random.fold_in(own_key, 1), dims, 0, int(grid[amount - 1]))
    grade = jnp.searchsorted(jnp.asarray(grid, jnp.int32), ticket, side="right")
    return jax.random.permutation(jax.random.fold_in(own_key, 2), amount)[grade].astype(jnp.int32)


def gaussian(stream_key, shape, scale, most, shards=(), kind=jnp.bfloat16):
    result = scale * jax.random.normal(stream_key, shape, jnp.float32)
    if shards:
        result = result * level_of(stream_key, shape, shards, -0.22, 0.18)
    return jnp.clip(result, -most, most).astype(kind)


def setup_inputs(seed: int = 0) -> dict:
    streams_of = jax.random.split(jax.random.key(seed), 8)
    hidden = draw_hidden(jax.random.fold_in(streams_of[7], 71), 0)
    out_weight = draw_out_weight(jax.random.fold_in(streams_of[7], 71), 0)
    targets = place_ends(ranked_ids(streams_of[2], (MB, SEQS, L), VOC, 2), jax.random.fold_in(streams_of[2], 3), 0, VOC - 1).astype(jnp.int32)
    prompt_start = place_ends(jax.random.randint(streams_of[3], (MB, SEQS), 0, L // 4), jax.random.fold_in(streams_of[3], 1), 0, (L // 4) - 1).astype(jnp.int32)
    response_len = draw_response_len(jax.random.fold_in(streams_of[7], 71), 0)
    partner = draw_partner(jax.random.fold_in(streams_of[7], 71), 0)
    ref_scores = gaussian(streams_of[6], (MB, SEQS), 10.0, 60.0, ((1, 8),), jnp.float32)
    return {"hidden": hidden, "out_weight": out_weight, "targets": targets, "prompt_start": prompt_start, "response_len": response_len, "partner": partner, "ref_scores": ref_scores}


margin_beta = 0.1
loss_scale = 65536.0


def reference(hidden, out_weight, targets, prompt_start, response_len, partner, ref_scores):
    weight_wide = out_weight.astype(jnp.float32)
    flat_hidden = hidden.reshape(MB * SEQS, L, D)
    flat_targets = targets.reshape(MB * SEQS, L)
    position = jnp.arange(L, dtype=jnp.int32)
    first_pos = prompt_start.reshape(MB * SEQS, 1)
    end_pos = (prompt_start + response_len).reshape(MB * SEQS, 1)
    response_mask = ((position[None, :] >= first_pos) & (position[None, :] < end_pos)).astype(jnp.float32)
    vocab_ids = jnp.arange(VOC, dtype=jnp.int32)

    def seq_logits(seq_hidden):
        return jnp.dot(seq_hidden.astype(jnp.float32), weight_wide, precision=lax.Precision.HIGHEST)

    def forward(element):
        seq_hidden, seq_targets = element
        logits = seq_logits(seq_hidden)
        row_peak = jnp.max(logits, axis=1)
        log_total = row_peak + jnp.log(jnp.sum(jnp.exp(logits - row_peak[:, None]), axis=1))
        picked = jnp.sum(jnp.where(seq_targets[:, None] == vocab_ids[None, :], logits, 0.0), axis=1)
        return picked - log_total, log_total

    token_logp, log_total = lax.map(forward, (flat_hidden, flat_targets))
    seq_sum = jnp.sum(response_mask * token_logp, axis=1).reshape(MB, SEQS)
    mean_length = jnp.sum(response_len).astype(jnp.float32) / (MB * SEQS)
    score_gap = seq_sum / mean_length - ref_scores
    partner_gap = jnp.take_along_axis(score_gap, partner, axis=1)
    seq_index = jnp.arange(SEQS, dtype=jnp.int32)
    pair_sign = jnp.where(seq_index[None, :] < partner, 1.0, -1.0)
    margin = margin_beta * pair_sign * (score_gap - partner_gap)
    pair_loss = jax.nn.softplus(-margin)
    seq_weight = -loss_scale * margin_beta * pair_sign * jax.nn.sigmoid(-margin) / mean_length
    row_weight = seq_weight.reshape(MB * SEQS, 1) * response_mask

    def backward(element):
        seq_hidden, seq_targets, seq_total, seq_rows = element
        logits = seq_logits(seq_hidden)
        softmax = jnp.exp(logits - seq_total[:, None])
        onehot = (seq_targets[:, None] == vocab_ids[None, :]).astype(jnp.float32)
        grad_logits = (seq_rows[:, None] * (onehot - softmax)).astype(jnp.bfloat16)
        return jnp.dot(grad_logits.astype(jnp.float32), weight_wide.T, precision=lax.Precision.HIGHEST)

    grad_hidden = lax.map(backward, (flat_hidden, flat_targets, log_total, row_weight))
    return pair_loss, grad_hidden.reshape(MB, SEQS, L, D)
```

```python
import functools

import jax
import jax.numpy as jnp
from jax import lax
from jax.experimental import pallas as pl
from jax.experimental.pallas import tpu as pltpu
from jax.sharding import PartitionSpec as P

margin_beta = 0.1
loss_scale = 65536.0
len_base = 17
len_span = 64
lane = 128
NEG = -1e30
F32 = jnp.float32
BF16 = jnp.bfloat16


def round_up(value, step):
    return -(-value // step) * step


def block_cols(cols):
    for size in (512, 640, 384, 256):
        if cols % size == 0:
            return size
    return lane


def gather_blocks(zid, ws, full):
    planes, pair, _ = full.shape
    depth = pair // 2
    core = zid[planes]
    for k in range(planes):
        mine = pl.multiple_of(core * depth, depth)
        other = pl.multiple_of((1 - core) * depth, depth)
        full[zid[k], pl.ds(mine, depth), :] = ws[k][...]
        full[zid[k], pl.ds(other, depth), :] = ws[planes + k][...]


def logits_block(h, full, start, width):
    acc = None
    for b in range(full.shape[0]):
        part = jnp.dot(h[b], full[b, :, pl.ds(start, width)], preferred_element_type=F32)
        acc = part if acc is None else acc + part
    return acc


def fold(x, op):
    out = x[:, :lane]
    for i in range(lane, x.shape[1], lane):
        out = op(out, x[:, i : i + lane])
    return out


def hits(info, tgt, start, width, padded):
    local = lax.broadcasted_iota(jnp.int32, (1, width), 1) + start
    onehot = (tgt[:, :] - info[0]) == local
    if padded:
        onehot = onehot & (local < info[1])
    return onehot


def mask_pad(info, x, start, padded):
    if not padded:
        return x
    local = lax.broadcasted_iota(jnp.int32, (1, x.shape[1]), 1) + start
    return jnp.where(local < info[1], x, NEG)


def nt_dot(a, b):
    return lax.dot_general(a, b, (((1,), (1,)), ((), ())), preferred_element_type=F32)


def pack_cols(cols, rows):
    lanes = lax.broadcasted_iota(jnp.int32, (rows, lane), 1)
    out = jnp.zeros((rows, lane), F32)
    for i, col in enumerate(cols):
        out = jnp.where(lanes == i, col, out)
    return out


def chunk_kernel(count, width, padded, carry, zid, info, h, tgt, *refs):
    before, refs = refs[:carry], refs[carry:]
    ws, (a, t, st, lg, mx, full) = refs[:count], refs[count:]
    planes = full.shape[0]

    @pl.when(pl.program_id(0) == 0)
    def _():
        gather_blocks(zid, ws, full)

    rows, cols = lg.shape
    steps = cols // width
    mx[...] = jnp.full(mx.shape, NEG, F32)

    def forward(j, state):
        start = pl.multiple_of(j * width, lane)
        x = mask_pad(info, logits_block(h, full, start, width), start, padded)
        lg[:, pl.ds(start, width)] = x
        mx[...] = jnp.maximum(mx[...], fold(x, jnp.maximum))
        return state

    lax.fori_loop(0, steps, forward, 0)
    peak = jnp.max(mx[...], axis=1, keepdims=True)
    total = jnp.zeros((rows, 1), F32)
    picked = jnp.zeros((rows, 1), F32)
    if carry:
        a_in, t_in, st_in = before
        old = st_in[:, 0:1]
        peak = jnp.maximum(peak, old)
        scale = jnp.exp(old - peak)
        total = st_in[:, 1:2] * scale
        picked = st_in[:, 2:3]
        for b in range(planes):
            a[b] = a_in[b] * scale
            t[b] = t_in[b]
    else:
        a[...] = jnp.zeros(a.shape, F32)
        t[...] = jnp.zeros(t.shape, t.dtype)

    def backward(j, state):
        total, picked = state
        start = pl.multiple_of(j * width, lane)
        x = lg[:, pl.ds(start, width)]
        e = jnp.exp(x - peak)
        onehot = hits(info, tgt, start, width, padded)
        total = total + jnp.sum(fold(e, jnp.add), axis=1, keepdims=True)
        hit = fold(jnp.where(onehot, x, 0.0), jnp.add)
        picked = picked + jnp.sum(hit, axis=1, keepdims=True)
        eb = e.astype(BF16)
        ob = jnp.where(onehot, 1.0, 0.0).astype(BF16)
        for b in range(planes):
            wj = full[b, :, pl.ds(start, width)]
            a[b] += nt_dot(eb, wj)
            t[b] += nt_dot(ob, wj).astype(t.dtype)
        return total, picked

    total, picked = lax.fori_loop(0, steps, backward, (total, picked))
    st[...] = pack_cols([peak, total, picked], rows)


def last_kernel(count, padded, zid, info, h, tgt, st_a, *refs):
    ws, (lg, st_t, full) = refs[:count], refs[count:]
    rows, cols = lg.shape

    @pl.when(pl.program_id(0) == 0)
    def _():
        gather_blocks(zid, ws, full)

    x = mask_pad(info, logits_block(h, full, 0, cols), 0, padded)
    lg[...] = x
    m_a, s_a, t_a = (st_a[:, i : i + 1] for i in range(3))
    m = jnp.maximum(m_a, jnp.max(fold(x, jnp.maximum), axis=1, keepdims=True))
    total = s_a * jnp.exp(m_a - m) + jnp.sum(fold(jnp.exp(x - m), jnp.add), axis=1, keepdims=True)
    onehot = hits(info, tgt, 0, cols, padded)
    picked = t_a + jnp.sum(fold(jnp.where(onehot, x, 0.0), jnp.add), axis=1, keepdims=True)
    packed = pack_cols([m, total, picked, m_a], rows)
    extra = st_t.shape[1] - rows
    if extra:
        packed = jnp.concatenate([packed, jnp.zeros((extra, lane), F32)], axis=0)
    st_t[...] = packed.T[:8]


def merge_stats(x, y):
    peak = jnp.maximum(x[0:1], y[0:1])
    total = x[1:2] * jnp.exp(x[0:1] - peak) + y[1:2] * jnp.exp(y[0:1] - peak)
    return jnp.concatenate([peak, total, x[2:3] + y[2:3], x[3:]], axis=0)


def finish_kernel(
    micro, count, padded, spans, zid, info, qid, a, t, lg, tgt, facts, own, merged, *refs
):
    ws, refs = refs[:count], refs[count:]
    outs, (loss, coef, full) = refs[:-3], refs[-3:]
    rows = a.shape[1]

    @pl.when(pl.program_id(0) == 0)
    def _():
        gather_blocks(zid, ws, full)
        before_peak = own[3:4]
        log_total = merged[0:1] + jnp.log(merged[1:2])
        picked = merged[2:3]
        seqs = facts.shape[0]
        ref_score, partner, lens, own_len = (facts[:, lane + i : lane + i + 1] for i in range(4))
        sub = lax.broadcasted_iota(jnp.int32, (seqs, own.shape[1]), 0)
        place = lax.broadcasted_iota(jnp.int32, (seqs, own.shape[1]), 1)
        limit = own_len.astype(jnp.int32)
        inside = jnp.zeros(sub.shape, jnp.bool_)
        for s, (low, cap) in enumerate(spans):
            here = place - low
            inside = inside | ((sub == s) & (here >= 0) & (here < cap) & (here < limit))
        token = jnp.where(inside, picked - log_total, 0.0)
        seq_sum = jnp.sum(token, axis=1, keepdims=True)
        mean_length = jnp.sum(lens, axis=0, keepdims=True) / (micro * seqs)
        gap = seq_sum / mean_length - ref_score
        row_id = lax.broadcasted_iota(jnp.int32, (seqs, seqs), 0)
        col_id = lax.broadcasted_iota(jnp.int32, (seqs, seqs), 1)
        gap_row = jnp.sum(jnp.where(row_id == col_id, gap, 0.0), axis=0, keepdims=True)
        mate = partner.astype(jnp.int32)
        mate_gap = jnp.sum(jnp.where(mate == col_id, gap_row, 0.0), axis=1, keepdims=True)
        own_id = lax.broadcasted_iota(jnp.int32, (seqs, 1), 0)
        sign = jnp.where(own_id < mate, 1.0, -1.0)
        margin = margin_beta * sign * (gap - mate_gap)
        value = jnp.maximum(-margin, 0.0) + jnp.log1p(jnp.exp(-jnp.abs(margin)))
        loss[...] = jnp.broadcast_to(value, loss.shape)
        slope = 1.0 / (1.0 + jnp.exp(margin))
        weight = -loss_scale * margin_beta * sign * slope / mean_length
        row_weight = jnp.sum(jnp.where(inside, weight, 0.0), axis=0, keepdims=True)
        soft = -row_weight * jnp.exp(before_peak - log_total)
        sub = lax.broadcasted_iota(jnp.int32, (lane, own.shape[1]), 0)
        both = jnp.where(sub == 0, row_weight, jnp.where(sub == 1, soft, log_total))
        coef[...] = both.T

    start = pl.multiple_of(pl.program_id(0) * rows, 8)
    hot = coef[pl.ds(start, rows), 0:1]
    soft = coef[pl.ds(start, rows), 1:2]
    level = coef[pl.ds(start, rows), 2:3]
    onehot = hits(info, tgt, 0, lg.shape[1], padded)
    soft_last = jnp.exp(lg[...] - level)
    grad = (hot * (jnp.where(onehot, 1.0, 0.0) - soft_last)).astype(BF16)
    for k, out in enumerate(outs):
        b = qid[k]
        new = nt_dot(grad, full[b])
        out[...] = (hot * t[b].astype(F32) + soft * a[b] + new).astype(BF16)


def plane_kernel(count, offs, *refs):
    parts, outs, buf = refs[:count], refs[count:-1], refs[-1]
    rows, win = parts[0].shape[0], outs[0].shape[0]
    acc = parts[0][...].astype(F32)
    for part in parts[1:]:
        acc = acc + part[...].astype(F32)
    buf[:rows] = acc
    buf[rows:] = jnp.zeros((win, acc.shape[1]), F32)
    for k, out in enumerate(outs):
        out[...] = buf[pl.ds(pl.multiple_of(offs[k], 8), win), :].astype(BF16)


def place_kernel(count, info, *refs):
    parts, out = refs[:count], refs[count]
    win = parts[0].shape[0]
    length = out.shape[2]
    for side in range(2):
        acc = parts[side][...].astype(F32)
        for part in parts[side + 2 :: 2]:
            acc = acc + part[...].astype(F32)
        rows = lax.broadcasted_iota(jnp.int32, acc.shape, 0)
        x = jnp.where(rows < info[3 + side], acc, 0.0)
        x = jnp.concatenate([x, jnp.zeros((length - win, x.shape[1]), F32)], axis=0)
        x = pltpu.roll(x, info[1 + side], 0)
        micro = info[0] if side == 0 else 1 - info[0]
        out[micro, 0] = x


SMEM = pl.BlockSpec(memory_space=pltpu.SMEM)
WHOLE = pl.BlockSpec(memory_space=pltpu.VMEM)


def params():
    return pltpu.CompilerParams(
        dimension_semantics=("arbitrary",), vmem_limit_bytes=60 * 1024 * 1024
    )


def body(dp, vocab, hidden, out_weight, targets, prompt_start, response_len, partner, ref_scores):
    micro, _, length, model = hidden.shape
    planes = dp // 2
    depth, cols = out_weight.shape
    quarter = model // vocab
    d = lax.axis_index("dp")
    v = lax.axis_index("vocab")
    core = d % 2
    z = d // 2
    caps = [round_up(len_base - 1 + len_span * (s + 1) // dp, 8) for s in range(dp)]
    win = max(caps)
    offsets = [sum(caps[:s]) for s in range(dp)]
    rows = sum(caps)
    row_block = rows
    if rows > 512:
        rows = round_up(rows, lane)
        row_block = lane
    grid = rows // row_block
    tail = rows - sum(caps)
    lanes = round_up(rows, lane)

    tiles = round_up(-(-cols // lane), planes) // planes
    last_tiles = max(1, tiles // 8)
    first_tiles = tiles // 4
    sizes = [first_tiles, tiles - first_tiles - last_tiles, last_tiles]
    chunk_cols = [size * lane for size in sizes if size]
    chunk_starts = [sum(chunk_cols[:i]) for i in range(len(chunk_cols))]
    chip_cols = tiles * lane
    padded = chip_cols * planes != cols
    weight = out_weight
    if padded:
        weight = jnp.pad(weight, ((0, 0), (0, chip_cols * planes - cols)))

    dp_swap = {k: [(i, i ^ k) for i in range(dp)] for k in range(1, dp)}

    def over_dp(x, k):
        return x if k == 0 else lax.ppermute(x, "dp", dp_swap[k])

    def piece(k, chunk, base):
        start = (base ^ k) * chip_cols + chunk_starts[chunk]
        return lax.dynamic_slice(weight, (0, start), (depth, chunk_cols[chunk]))

    order = sorted(range(planes), key=lambda k: (k != 0, k != 1, -k))
    pieces = [piece(k, 0, z) for k in order]
    pieces, v_hid = lax.optimization_barrier((pieces, v))
    sent = {(0, k): over_dp(x, 2 * k) for k, x in zip(order, pieces)}

    windows, facts = [], []
    lens_total = jnp.sum(response_len).astype(F32)
    for m in range(micro):
        start = prompt_start[m, 0]
        windows.append(
            lax.dynamic_slice(hidden[m, 0], (start, v_hid * quarter), (win, quarter))
        )
        ids = lax.dynamic_slice(targets[m, 0], (start,), (win,)).astype(F32)
        first = jnp.pad(ids, (0, lane - win))[None]
        second = jnp.stack(
            [ref_scores[m, 0], partner[m, 0].astype(F32), lens_total, response_len[m, 0].astype(F32)]
        )
        facts.append(jnp.concatenate([first, jnp.pad(second, (0, lane - 4))[None]], axis=1))

    def by_core(pair):
        flip = core == 0
        return jnp.where(flip, pair[0], pair[1]), jnp.where(flip, pair[1], pair[0])

    window_pair, fact_pair = by_core(windows), by_core(facts)
    window_pair, z_rest = lax.optimization_barrier((window_pair, z))
    window_all = jnp.zeros((dp, win, quarter), BF16)
    fact_all = jnp.zeros((dp, 2 * lane), F32)
    for k in range(dp):
        got = over_dp(window_pair[k % 2], k)
        window_all = lax.dynamic_update_slice(window_all, got[None], (d ^ k, 0, 0))
        fact = over_dp(fact_pair[k % 2], k)
        fact_all = lax.dynamic_update_slice(fact_all, fact, (d ^ k, 0))

    for chunk in range(1, len(chunk_cols)):
        for k in order:
            sent[chunk, k] = over_dp(piece(k, chunk, z_rest), 2 * k)

    def chunk_blocks(chunk, after=None):
        mine = [sent[chunk, k] for k in range(planes)]
        if after is not None:
            mine, after = lax.optimization_barrier((mine, after))
        return mine + [over_dp(x, 1) for x in mine], after

    zid = jnp.stack([z ^ k for k in range(planes)] + [core]).astype(jnp.int32)
    chip_start = z * chip_cols
    infos = [
        jnp.stack([v * cols + chip_start + off, cols - chip_start - off]).astype(jnp.int32)
        for off in chunk_starts
    ]

    full = jnp.concatenate(
        [window_all[s, : caps[s]] for s in range(dp)]
        + ([jnp.zeros((tail, quarter), BF16)] if tail else []),
        axis=0,
    )
    full = lax.optimization_barrier(full)
    bit = 1
    while bit < vocab:
        got = lax.ppermute(full, "vocab", [(i, i ^ bit) for i in range(vocab)])
        full = jnp.where(
            (v & bit) == 0,
            jnp.concatenate([full, got], axis=1),
            jnp.concatenate([got, full], axis=1),
        )
        bit *= 2
    full = lax.optimization_barrier(full)
    h = full.reshape(rows, planes, 2 * depth).transpose(1, 0, 2)

    def row_facts(make, fill):
        parts = [make(s)[: caps[s]] for s in range(dp)]
        if tail:
            parts.append(jnp.full((tail,), fill, F32))
        return jnp.concatenate(parts)

    tgt = row_facts(lambda s: fact_all[s, :win], -1.0).astype(jnp.int32).reshape(rows, 1)
    row_spec = lambda *shape: pl.BlockSpec((*shape[:-2], row_block, shape[-1]), lambda i: (0,) * (len(shape) - 2) + (i, 0))
    h_spec = row_spec(planes, rows, 2 * depth)
    a_shape = jax.ShapeDtypeStruct((planes, rows, 2 * depth), F32)
    t_shape = jax.ShapeDtypeStruct((planes, rows, 2 * depth), BF16)
    st_shape = jax.ShapeDtypeStruct((rows, lane), F32)
    stt_shape = jax.ShapeDtypeStruct((8, lanes), F32)
    col_spec = row_spec(rows, 1)
    st_spec = row_spec(rows, lane)
    w_specs = [WHOLE] * dp

    state = ()
    for chunk, size in enumerate(chunk_cols[:-1]):
        blocks_in, _ = chunk_blocks(chunk, state[2] if state else None)
        carry = len(state)
        state = pl.pallas_call(
            functools.partial(chunk_kernel, dp, block_cols(size), padded, carry),
            grid=(grid,),
            in_specs=[SMEM, SMEM, h_spec, col_spec, *[h_spec, h_spec, st_spec][:carry], *w_specs],
            out_specs=[h_spec, h_spec, st_spec],
            out_shape=[a_shape, t_shape, st_shape],
            input_output_aliases={4: 0, 5: 1, 6: 2} if carry else {},
            scratch_shapes=[
                pltpu.VMEM((row_block, size), F32),
                pltpu.VMEM((row_block, lane), F32),
                pltpu.VMEM((planes, 2 * depth, size), BF16),
            ],
            compiler_params=params(),
            name="chunk",
        )(zid, infos[chunk], h, tgt, *state, *blocks_in)
    a, t, st_a = state
    last, st_a = chunk_blocks(len(chunk_cols) - 1, st_a)

    last_cols = chunk_cols[-1]
    full_scratch = pltpu.VMEM((planes, 2 * depth, last_cols), BF16)
    lg, st_t = pl.pallas_call(
        functools.partial(last_kernel, dp, padded),
        grid=(grid,),
        in_specs=[SMEM, SMEM, h_spec, col_spec, st_spec, *w_specs],
        out_specs=[row_spec(rows, last_cols), pl.BlockSpec((8, lanes // grid), lambda i: (0, i))],
        out_shape=[jax.ShapeDtypeStruct((rows, last_cols), F32), stt_shape],
        scratch_shapes=[full_scratch],
        compiler_params=params(),
        name="last",
    )(zid, infos[-1], h, tgt, st_a, *last)

    merged = st_t
    hops = [("vocab", 1 << i) for i in range(vocab.bit_length() - 1)]
    hops += [("dp", 2 << i) for i in range(planes.bit_length() - 1)]
    for axis, bit in hops:
        size = vocab if axis == "vocab" else dp
        merged = merge_stats(merged, lax.ppermute(merged, axis, [(i, i ^ bit) for i in range(size)]))

    qid = jnp.stack([v ^ k for k in range(vocab)]).astype(jnp.int32)
    part_shape = jax.ShapeDtypeStruct((rows, quarter), BF16)
    *parts, loss = pl.pallas_call(
        functools.partial(finish_kernel, micro, dp, padded, tuple(zip(offsets, caps))),
        grid=(grid,),
        in_specs=[SMEM, SMEM, SMEM, h_spec, h_spec, row_spec(rows, last_cols), col_spec]
        + [WHOLE] * 3
        + w_specs,
        out_specs=[row_spec(rows, quarter)] * vocab + [pl.BlockSpec((dp, lane), lambda i: (0, 0))],
        out_shape=[part_shape] * vocab + [jax.ShapeDtypeStruct((dp, lane), F32)],
        scratch_shapes=[pltpu.VMEM((lanes, lane), F32), full_scratch],
        compiler_params=params(),
        name="finish",
    )(zid, infos[-1], qid, a, t, lg, tgt, fact_all, st_t, merged, *last)

    gathered = [parts[0]] + [
        lax.ppermute(parts[k], "vocab", [(i, i ^ k) for i in range(vocab)]) for k in range(1, vocab)
    ]
    offs = sum(
        jnp.where((d ^ jnp.arange(dp, dtype=jnp.int32)) == s, offsets[s], 0) for s in range(dp)
    ).astype(jnp.int32)
    out_shape = jax.ShapeDtypeStruct((win, quarter), BF16)
    shares = pl.pallas_call(
        functools.partial(plane_kernel, vocab),
        in_specs=[SMEM] + [WHOLE] * vocab,
        out_specs=[WHOLE] * dp,
        out_shape=[out_shape] * dp,
        scratch_shapes=[pltpu.VMEM((rows + win, quarter), F32)],
        name="plane",
    )(offs, *gathered)
    finals = [over_dp(shares[k], k) for k in range(dp)]
    own_start, other_start = by_core([prompt_start[0, 0], prompt_start[1, 0]])
    own_len, other_len = by_core([response_len[0, 0], response_len[1, 0]])
    info = jnp.stack([core, own_start, other_start, own_len, other_len]).astype(jnp.int32)
    grad = pl.pallas_call(
        functools.partial(place_kernel, dp),
        in_specs=[SMEM] + [WHOLE] * dp,
        out_specs=WHOLE,
        out_shape=jax.ShapeDtypeStruct((micro, 1, length, quarter), F32),
        name="place",
    )(info, *finals)

    other_loss = over_dp(loss, 1)
    pair = by_core([loss, other_loss])
    pair_loss = jnp.stack([lax.dynamic_slice(x, (d, 0), (1, 1))[0] for x in pair])
    return pair_loss, grad


def solution(mesh):
    return jax.shard_map(
        functools.partial(body, mesh.shape["dp"], mesh.shape["vocab"]),
        mesh=mesh,
        in_specs=(
            P(None, "dp", None, None),
            P("dp", "vocab"),
            P(None, "dp", None),
            P(None, "dp"),
            P(None, "dp"),
            P(None, "dp"),
            P(None, "dp"),
        ),
        out_specs=(P(None, "dp"), P(None, "dp", None, "vocab")),
        check_vma=False,
    )
```

```python
import functools

import jax
import jax.numpy as jnp
from jax import lax
from jax.experimental import pallas as pl
from jax.experimental.pallas import tpu as pltpu
from jax.sharding import PartitionSpec as P


margin_beta = 0.1
loss_scale = 65536.0
len_base = 17
len_span = 64
lane = 128
NEG = -1e30
F32 = jnp.float32
BF16 = jnp.bfloat16


def round_up(value, step):
    return -(-value // step) * step


def block_cols(cols):
    for size in (512, 640, 384, 256):
        if cols % size == 0:
            return size
    return lane


def gather_blocks(zid, ws, full):
    planes, pair, _ = full.shape
    depth = pair // 2
    core = zid[planes]
    for k in range(planes):
        mine = pl.multiple_of(core * depth, depth)
        other = pl.multiple_of((1 - core) * depth, depth)
        full[zid[k], pl.ds(mine, depth), :] = ws[k][...]
        full[zid[k], pl.ds(other, depth), :] = ws[planes + k][...]


def logits_block(h, full, start, width):
    acc = None
    for b in range(full.shape[0]):
        part = jnp.dot(h[b], full[b, :, pl.ds(start, width)], preferred_element_type=F32)
        acc = part if acc is None else acc + part
    return acc


def fold(x, op):
    out = x[:, :lane]
    for i in range(lane, x.shape[1], lane):
        out = op(out, x[:, i : i + lane])
    return out


def hits(info, tgt, start, width, padded):
    local = lax.broadcasted_iota(jnp.int32, (1, width), 1) + start
    onehot = (tgt[:, :] - info[0]) == local
    if padded:
        onehot = onehot & (local < info[1])
    return onehot


def mask_pad(info, x, start, padded):
    if not padded:
        return x
    local = lax.broadcasted_iota(jnp.int32, (1, x.shape[1]), 1) + start
    return jnp.where(local < info[1], x, NEG)


def nt_dot(a, b):
    return lax.dot_general(a, b, (((1,), (1,)), ((), ())), preferred_element_type=F32)


def pack_cols(cols, rows):
    lanes = lax.broadcasted_iota(jnp.int32, (rows, lane), 1)
    out = jnp.zeros((rows, lane), F32)
    for i, col in enumerate(cols):
        out = jnp.where(lanes == i, col, out)
    return out


def chunk_kernel(count, width, padded, carry, zid, info, h, tgt, *refs):
    before, refs = refs[:carry], refs[carry:]
    ws, (a, t, st, lg, mx, full) = refs[:count], refs[count:]
    planes = full.shape[0]

    @pl.when(pl.program_id(0) == 0)
    def _():
        gather_blocks(zid, ws, full)

    rows, cols = lg.shape
    steps = cols // width
    mx[...] = jnp.full(mx.shape, NEG, F32)

    def forward(j, state):
        start = pl.multiple_of(j * width, lane)
        x = mask_pad(info, logits_block(h, full, start, width), start, padded)
        lg[:, pl.ds(start, width)] = x
        mx[...] = jnp.maximum(mx[...], fold(x, jnp.maximum))
        return state

    lax.fori_loop(0, steps, forward, 0)
    peak = jnp.max(mx[...], axis=1, keepdims=True)
    total = jnp.zeros((rows, 1), F32)
    picked = jnp.zeros((rows, 1), F32)
    if carry:
        a_in, t_in, st_in = before
        old = st_in[:, 0:1]
        peak = jnp.maximum(peak, old)
        scale = jnp.exp(old - peak)
        total = st_in[:, 1:2] * scale
        picked = st_in[:, 2:3]
        for b in range(planes):
            a[b] = a_in[b] * scale
            t[b] = t_in[b]
    else:
        a[...] = jnp.zeros(a.shape, F32)
        t[...] = jnp.zeros(t.shape, t.dtype)

    def backward(j, state):
        total, picked = state
        start = pl.multiple_of(j * width, lane)
        x = lg[:, pl.ds(start, width)]
        e = jnp.exp(x - peak)
        onehot = hits(info, tgt, start, width, padded)
        total = total + jnp.sum(fold(e, jnp.add), axis=1, keepdims=True)
        hit = fold(jnp.where(onehot, x, 0.0), jnp.add)
        picked = picked + jnp.sum(hit, axis=1, keepdims=True)
        eb = e.astype(BF16)
        ob = jnp.where(onehot, 1.0, 0.0).astype(BF16)
        for b in range(planes):
            wj = full[b, :, pl.ds(start, width)]
            a[b] += nt_dot(eb, wj)
            t[b] += nt_dot(ob, wj).astype(t.dtype)
        return total, picked

    total, picked = lax.fori_loop(0, steps, backward, (total, picked))
    st[...] = pack_cols([peak, total, picked], rows)


def last_kernel(count, padded, zid, info, h, tgt, st_a, *refs):
    ws, (lg, st_t, full) = refs[:count], refs[count:]
    rows, cols = lg.shape

    @pl.when(pl.program_id(0) == 0)
    def _():
        gather_blocks(zid, ws, full)

    x = mask_pad(info, logits_block(h, full, 0, cols), 0, padded)
    lg[...] = x
    m_a, s_a, t_a = (st_a[:, i : i + 1] for i in range(3))
    m = jnp.maximum(m_a, jnp.max(fold(x, jnp.maximum), axis=1, keepdims=True))
    total = s_a * jnp.exp(m_a - m) + jnp.sum(fold(jnp.exp(x - m), jnp.add), axis=1, keepdims=True)
    onehot = hits(info, tgt, 0, cols, padded)
    picked = t_a + jnp.sum(fold(jnp.where(onehot, x, 0.0), jnp.add), axis=1, keepdims=True)
    packed = pack_cols([m, total, picked, m_a], rows)
    extra = st_t.shape[1] - rows
    if extra:
        packed = jnp.concatenate([packed, jnp.zeros((extra, lane), F32)], axis=0)
    st_t[...] = packed.T[:8]


def merge_stats(x, y):
    peak = jnp.maximum(x[0:1], y[0:1])
    total = x[1:2] * jnp.exp(x[0:1] - peak) + y[1:2] * jnp.exp(y[0:1] - peak)
    return jnp.concatenate([peak, total, x[2:3] + y[2:3], x[3:]], axis=0)


def finish_kernel(
    micro, count, padded, spans, zid, info, qid, a, t, lg, tgt, facts, own, merged, *refs
):
    ws, refs = refs[:count], refs[count:]
    outs, (loss, coef, full) = refs[:-3], refs[-3:]
    rows = a.shape[1]

    @pl.when(pl.program_id(0) == 0)
    def _():
        gather_blocks(zid, ws, full)
        before_peak = own[3:4]
        log_total = merged[0:1] + jnp.log(merged[1:2])
        picked = merged[2:3]
        seqs = facts.shape[0]
        terms = [facts[:, lane + i : lane + i + 1] for i in range(6)]
        ref_score, partner, lens, own_len = terms[0] + terms[1] + terms[2], *terms[3:]
        sub = lax.broadcasted_iota(jnp.int32, (seqs, own.shape[1]), 0)
        place = lax.broadcasted_iota(jnp.int32, (seqs, own.shape[1]), 1)
        limit = own_len.astype(jnp.int32)
        inside = jnp.zeros(sub.shape, jnp.bool_)
        for s, (low, cap) in enumerate(spans):
            here = place - low
            inside = inside | ((sub == s) & (here >= 0) & (here < cap) & (here < limit))
        token = jnp.where(inside, picked - log_total, 0.0)
        seq_sum = jnp.sum(token, axis=1, keepdims=True)
        mean_length = jnp.sum(lens, axis=0, keepdims=True) / (micro * seqs)
        gap = seq_sum / mean_length - ref_score
        row_id = lax.broadcasted_iota(jnp.int32, (seqs, seqs), 0)
        col_id = lax.broadcasted_iota(jnp.int32, (seqs, seqs), 1)
        gap_row = jnp.sum(jnp.where(row_id == col_id, gap, 0.0), axis=0, keepdims=True)
        mate = partner.astype(jnp.int32)
        mate_gap = jnp.sum(jnp.where(mate == col_id, gap_row, 0.0), axis=1, keepdims=True)
        own_id = lax.broadcasted_iota(jnp.int32, (seqs, 1), 0)
        sign = jnp.where(own_id < mate, 1.0, -1.0)
        margin = margin_beta * sign * (gap - mate_gap)
        value = jnp.maximum(-margin, 0.0) + jnp.log1p(jnp.exp(-jnp.abs(margin)))
        loss[...] = jnp.broadcast_to(value, loss.shape)
        slope = 1.0 / (1.0 + jnp.exp(margin))
        weight = -loss_scale * margin_beta * sign * slope / mean_length
        row_weight = jnp.sum(jnp.where(inside, weight, 0.0), axis=0, keepdims=True)
        soft = -row_weight * jnp.exp(before_peak - log_total)
        chance = jnp.exp(jnp.minimum(picked - log_total, 0.0))
        rounded = (row_weight * (1.0 - chance)).astype(BF16).astype(F32)
        early = rounded + row_weight * chance
        sub = lax.broadcasted_iota(jnp.int32, (lane, own.shape[1]), 0)
        both = jnp.where(sub == 0, row_weight, jnp.where(sub == 1, soft, log_total))
        both = jnp.where(sub == 3, early, both)
        coef[...] = both.T

    start = pl.multiple_of(pl.program_id(0) * rows, 8)
    hot = coef[pl.ds(start, rows), 0:1]
    soft = coef[pl.ds(start, rows), 1:2]
    level = coef[pl.ds(start, rows), 2:3]
    early = coef[pl.ds(start, rows), 3:4]
    onehot = hits(info, tgt, 0, lg.shape[1], padded)
    soft_last = jnp.exp(lg[...] - level)
    grad = (hot * (jnp.where(onehot, 1.0, 0.0) - soft_last)).astype(BF16)
    for k, out in enumerate(outs):
        b = qid[k]
        new = nt_dot(grad, full[b])
        out[...] = (early * t[b].astype(F32) + soft * a[b] + new).astype(BF16)


def plane_kernel(count, offs, *refs):
    parts, outs, buf = refs[:count], refs[count:-1], refs[-1]
    rows, win = parts[0].shape[0], outs[0].shape[0]
    acc = parts[0][...].astype(F32)
    for part in parts[1:]:
        acc = acc + part[...].astype(F32)
    buf[:rows] = acc
    buf[rows:] = jnp.zeros((win, acc.shape[1]), F32)
    for k, out in enumerate(outs):
        out[...] = buf[pl.ds(pl.multiple_of(offs[k], 8), win), :].astype(BF16)


def place_kernel(count, info, *refs):
    parts, out = refs[:count], refs[count]
    win = parts[0].shape[0]
    length = out.shape[2]
    for side in range(2):
        acc = parts[side][...].astype(F32)
        for part in parts[side + 2 :: 2]:
            acc = acc + part[...].astype(F32)
        rows = lax.broadcasted_iota(jnp.int32, acc.shape, 0)
        x = jnp.where(rows < info[3 + side], acc, 0.0)
        x = jnp.concatenate([x, jnp.zeros((length - win, x.shape[1]), F32)], axis=0)
        x = pltpu.roll(x, info[1 + side], 0)
        micro = info[0] if side == 0 else 1 - info[0]
        out[micro, 0] = x


def open_kernel(index, ref, targets, hidden, *outs):
    micro, _, rows, _ = hidden.shape
    first_pos, length = ([index[2 + i * micro], index[3 + i * micro]] for i in range(2))
    quarter = outs[0].shape[1]
    win = outs[0].shape[0] - 8
    total = length[0] + length[1]
    for i, out in enumerate(outs):
        m = index[1] if i == 0 else 1 - index[1]
        first = jnp.where(m == 0, first_pos[0], first_pos[1])
        start = pl.multiple_of(index[0] * quarter, lane)
        x = hidden[m, 0, :, pl.ds(start, quarter)].astype(F32)
        out[:win] = pltpu.roll(x, rows - first, 0)[:win].astype(BF16)
        ids = jnp.broadcast_to(targets[m].astype(F32), (8, rows))
        ids = pltpu.roll(ids, rows - first, 1)[:, :lane].astype(jnp.int32)
        high = lax.shift_right_logical(ids, 8).astype(F32)
        low = (ids & 255).astype(F32)
        sub = lax.broadcasted_iota(jnp.int32, (8, lane), 0)
        lanes = lax.broadcasted_iota(jnp.int32, (8, lane), 1)
        left = jnp.full((8, lane), ref[m], F32)
        terms = []
        for _ in range(3):
            terms.append(left.astype(BF16).astype(F32))
            left = left - terms[-1]
        for scalar in (index[2 + 2 * micro + m], total, index[2 + micro + m]):
            terms.append(jnp.full((8, lane), scalar, jnp.int32).astype(F32))
        facts = jnp.zeros((8, lane), F32)
        for j, term in enumerate(terms):
            facts = jnp.where(lanes == j, term, facts)
        facts = jnp.where(sub == 2, facts, 0.0)
        facts = jnp.where(sub == 0, high, jnp.where(sub == 1, low, facts))
        if quarter > lane:
            facts = jnp.concatenate([facts, jnp.zeros((8, quarter - lane), F32)], axis=1)
        out[win:] = facts.astype(BF16)


def pack_kernel(count, spans, source, *refs):
    parts, (full, tgt, facts, buf, acc) = refs[:count], refs[count:]
    win = buf.shape[1] - 8
    for k in range(count):
        buf[source[k]] = parts[k][...].astype(F32)
    end = spans[-1][0] + spans[-1][1]
    for s, (low, cap) in enumerate(spans):
        acc[low : low + cap] = buf[s, :cap]
        facts[s : s + 1, :lane] = buf[s, win : win + 1, :lane] * 256.0 + buf[s, win + 1 : win + 2, :lane]
        facts[s : s + 1, lane:] = buf[s, win + 2 : win + 3, :lane]
    if end < acc.shape[0]:
        acc[end:] = jnp.zeros((acc.shape[0] - end, acc.shape[1]), F32)
        tgt[end:] = jnp.full((acc.shape[0] - end, 1), -1, jnp.int32)
    full[...] = acc[...].astype(BF16)
    ids = jnp.concatenate([facts[:, :lane], jnp.zeros((lane - count, lane), F32)], axis=0).T
    for s, (low, cap) in enumerate(spans):
        tgt[low : low + cap] = ids[:cap, s : s + 1].astype(jnp.int32)


SMEM = pl.BlockSpec(memory_space=pltpu.SMEM)
WHOLE = pl.BlockSpec(memory_space=pltpu.VMEM)


def params():
    return pltpu.CompilerParams(
        dimension_semantics=("arbitrary",), vmem_limit_bytes=60 * 1024 * 1024
    )


def program(dp, vocab, hidden, out_weight, targets, prompt_start, response_len, partner, ref_scores):
    micro, _, length, model = hidden.shape
    planes = dp // 2
    depth, cols = out_weight.shape
    quarter = model // vocab
    d = lax.axis_index("dp")
    v = lax.axis_index("vocab")
    core = d % 2
    z = d // 2
    caps = [round_up(len_base - 1 + len_span * (s + 1) // dp, 8) for s in range(dp)]
    win = max(caps)
    offsets = [sum(caps[:s]) for s in range(dp)]
    rows = sum(caps)
    row_block = rows
    if rows > 512:
        rows = round_up(rows, lane)
        row_block = lane
    grid = rows // row_block
    lanes = round_up(rows, lane)

    tiles = round_up(-(-cols // lane), planes) // planes
    last_tiles = max(1, tiles // 5)
    first_tiles = tiles // 2
    sizes = [first_tiles, tiles - first_tiles - last_tiles, last_tiles]
    chunk_cols = [size * lane for size in sizes if size]
    chunk_starts = [sum(chunk_cols[:i]) for i in range(len(chunk_cols))]
    chip_cols = tiles * lane
    padded = chip_cols * planes != cols
    weight = out_weight
    if padded:
        weight = jnp.pad(weight, ((0, 0), (0, chip_cols * planes - cols)))

    dp_swap = {k: [(i, i ^ k) for i in range(dp)] for k in range(1, dp)}

    def over_dp(x, k):
        return x if k == 0 else lax.ppermute(x, "dp", dp_swap[k])

    def piece(k, chunk, base):
        start = (base ^ k) * chip_cols + chunk_starts[chunk]
        return lax.dynamic_slice(weight, (0, start), (depth, chunk_cols[chunk]))

    def by_core(pair):
        flip = core == 0
        return jnp.where(flip, pair[0], pair[1]), jnp.where(flip, pair[1], pair[0])

    message = win + 8
    window_shape = jax.ShapeDtypeStruct((message, quarter), BF16)
    window_pair = pl.pallas_call(
        open_kernel,
        in_specs=[SMEM] * 2 + [WHOLE] * 2,
        out_specs=[WHOLE] * 2,
        out_shape=[window_shape] * 2,
        name="open",
    )(
        jnp.concatenate(
            [jnp.stack([v, core]).astype(jnp.int32)]
            + [x.reshape(-1) for x in (prompt_start, response_len, partner)]
        ),
        ref_scores.reshape(-1),
        targets,
        hidden,
    )
    window_pair, z_rest = lax.optimization_barrier((window_pair, z))
    spans = tuple(zip(offsets, caps))
    windows = [over_dp(window_pair[k % 2], k) for k in range(dp)]
    full, tgt, fact_all = pl.pallas_call(
        functools.partial(pack_kernel, dp, spans),
        in_specs=[SMEM] + [WHOLE] * dp,
        out_specs=[WHOLE] * 3,
        out_shape=[
            jax.ShapeDtypeStruct((rows, quarter), BF16),
            jax.ShapeDtypeStruct((rows, 1), jnp.int32),
            jax.ShapeDtypeStruct((dp, 2 * lane), F32),
        ],
        scratch_shapes=[
            pltpu.VMEM((dp, message, quarter), F32),
            pltpu.VMEM((rows, quarter), F32),
        ],
        name="pack",
    )(d ^ jnp.arange(dp, dtype=jnp.int32), *windows)

    order = sorted(range(planes), key=lambda k: (k != 0, k != 1, -k))
    sent = {}
    for chunk in range(len(chunk_cols)):
        for k in order:
            part = piece(k, chunk, z_rest)
            sent[chunk, k] = over_dp(part, 2 * k)

    def chunk_blocks(chunk, after=None):
        mine = [sent[chunk, k] for k in range(planes)]
        if after is not None:
            mine, after = lax.optimization_barrier((mine, after))
        return mine + [over_dp(x, 1) for x in mine], after

    zid = jnp.stack([z ^ k for k in range(planes)] + [core]).astype(jnp.int32)
    chip_start = z * chip_cols
    infos = [
        jnp.stack([v * cols + chip_start + off, cols - chip_start - off]).astype(jnp.int32)
        for off in chunk_starts
    ]

    bit = 1
    while bit < vocab:
        got = lax.ppermute(full, "vocab", [(i, i ^ bit) for i in range(vocab)])
        full = jnp.where(
            (v & bit) == 0,
            jnp.concatenate([full, got], axis=1),
            jnp.concatenate([got, full], axis=1),
        )
        bit *= 2
    full = lax.optimization_barrier(full)
    h = full.reshape(rows, planes, 2 * depth).transpose(1, 0, 2)

    row_spec = lambda *shape: pl.BlockSpec((*shape[:-2], row_block, shape[-1]), lambda i: (0,) * (len(shape) - 2) + (i, 0))
    h_spec = row_spec(planes, rows, 2 * depth)
    a_shape = jax.ShapeDtypeStruct((planes, rows, 2 * depth), F32)
    t_shape = jax.ShapeDtypeStruct((planes, rows, 2 * depth), BF16)
    st_shape = jax.ShapeDtypeStruct((rows, lane), F32)
    stt_shape = jax.ShapeDtypeStruct((8, lanes), F32)
    col_spec = row_spec(rows, 1)
    st_spec = row_spec(rows, lane)
    w_specs = [WHOLE] * dp

    state = ()
    for chunk, size in enumerate(chunk_cols[:-1]):
        blocks_in, _ = chunk_blocks(chunk, state[2] if state else None)
        carry = len(state)
        call = pl.pallas_call(
            functools.partial(chunk_kernel, dp, block_cols(size), padded, carry),
            grid=(grid,),
            in_specs=[SMEM, SMEM, h_spec, col_spec, *[h_spec, h_spec, st_spec][:carry], *w_specs],
            out_specs=[h_spec, h_spec, st_spec],
            out_shape=[a_shape, t_shape, st_shape],
            input_output_aliases={4: 0, 5: 1, 6: 2} if carry else {},
            scratch_shapes=[
                pltpu.VMEM((row_block, size), F32),
                pltpu.VMEM((row_block, lane), F32),
                pltpu.VMEM((planes, 2 * depth, size), BF16),
            ],
            compiler_params=params(),
            name="chunk",
        )
        state = call(zid, infos[chunk], h, tgt, *state, *blocks_in)
    a, t, st_a = state
    last, st_a = chunk_blocks(len(chunk_cols) - 1, st_a)

    last_cols = chunk_cols[-1]
    full_scratch = pltpu.VMEM((planes, 2 * depth, last_cols), BF16)
    lg, st_t = pl.pallas_call(
        functools.partial(last_kernel, dp, padded),
        grid=(grid,),
        in_specs=[SMEM, SMEM, h_spec, col_spec, st_spec, *w_specs],
        out_specs=[row_spec(rows, last_cols), pl.BlockSpec((8, lanes // grid), lambda i: (0, i))],
        out_shape=[jax.ShapeDtypeStruct((rows, last_cols), F32), stt_shape],
        scratch_shapes=[full_scratch],
        compiler_params=params(),
        name="last",
    )(zid, infos[-1], h, tgt, st_a, *last)

    merged = st_t
    hops = [("vocab", 1 << i) for i in range(vocab.bit_length() - 1)]
    hops += [("dp", 2 << i) for i in range(planes.bit_length() - 1)]
    for axis, bit in hops:
        size = vocab if axis == "vocab" else dp
        merged = merge_stats(merged, lax.ppermute(merged, axis, [(i, i ^ bit) for i in range(size)]))

    qid = jnp.stack([v ^ k for k in range(vocab)]).astype(jnp.int32)
    part_shape = jax.ShapeDtypeStruct((rows, quarter), BF16)
    *parts, loss = pl.pallas_call(
        functools.partial(finish_kernel, micro, dp, padded, spans),
        grid=(grid,),
        in_specs=[SMEM, SMEM, SMEM, h_spec, h_spec, row_spec(rows, last_cols), col_spec]
        + [WHOLE] * 3
        + w_specs,
        out_specs=[row_spec(rows, quarter)] * vocab + [pl.BlockSpec((dp, lane), lambda i: (0, 0))],
        out_shape=[part_shape] * vocab + [jax.ShapeDtypeStruct((dp, lane), F32)],
        scratch_shapes=[pltpu.VMEM((lanes, lane), F32), full_scratch],
        compiler_params=params(),
        name="finish",
    )(zid, infos[-1], qid, a, t, lg, tgt, fact_all, st_t, merged, *last)

    gathered = [parts[0]] + [
        lax.ppermute(parts[k], "vocab", [(i, i ^ k) for i in range(vocab)]) for k in range(1, vocab)
    ]
    offs = sum(
        jnp.where((d ^ jnp.arange(dp, dtype=jnp.int32)) == s, offsets[s], 0) for s in range(dp)
    ).astype(jnp.int32)
    out_shape = jax.ShapeDtypeStruct((win, quarter), BF16)
    shares = pl.pallas_call(
        functools.partial(plane_kernel, vocab),
        in_specs=[SMEM] + [WHOLE] * vocab,
        out_specs=[WHOLE] * dp,
        out_shape=[out_shape] * dp,
        scratch_shapes=[pltpu.VMEM((rows + win, quarter), F32)],
        name="plane",
    )(offs, *gathered)
    finals = [over_dp(shares[k], k) for k in range(dp)]
    own_start, other_start = by_core([prompt_start[0, 0], prompt_start[1, 0]])
    own_len, other_len = by_core([response_len[0, 0], response_len[1, 0]])
    info = jnp.stack([core, own_start, other_start, own_len, other_len]).astype(jnp.int32)
    grad = pl.pallas_call(
        functools.partial(place_kernel, dp),
        in_specs=[SMEM] + [WHOLE] * dp,
        out_specs=WHOLE,
        out_shape=jax.ShapeDtypeStruct((micro, 1, length, quarter), F32),
        name="place",
    )(info, *finals)

    other_loss = over_dp(loss, 1)
    pair = by_core([loss, other_loss])
    pair_loss = jnp.stack([lax.dynamic_slice(x, (d, 0), (1, 1))[0] for x in pair])
    return pair_loss, grad


def solution(mesh):
    return jax.shard_map(
        functools.partial(program, mesh.shape["dp"], mesh.shape["vocab"]),
        mesh=mesh,
        in_specs=(
            P(None, "dp", None, None),
            P("dp", "vocab"),
            P(None, "dp", None),
            P(None, "dp"),
            P(None, "dp"),
            P(None, "dp"),
            P(None, "dp"),
        ),
        out_specs=(P(None, "dp"), P(None, "dp", None, "vocab")),
        check_vma=False,
    )
```
